32 devices in a mesh: rows: 8 (over z, y), rep: 4 (over x, core).
Axes of the slice: x: 2, y: 2, z: 4, core: 2. Of those that a mesh axis runs over, the one named last changes fastest.
Arguments:
- binned: int32 [8192, 1024], P('rows', 'rep'), may hold values from 0 to 127
- gradients: bfloat16 [8192], P('rows'), may hold values from -3 to 3
- hessians: bfloat16 [8192], P('rows'), may hold values from 0.019897461 to 0.25
- parents: int32 [8192], P('rows'), may hold values from 0 to 15
- split_feature: int32 [16], replicated, may hold values from 0 to 1023
- split_bin: int32 [16], replicated, may hold values from 32 to 95
- elected: int32 [32, 512], P(None, 'rep'), may hold values from 0 to 255
Outputs:
- new_nodes: int32 [8192], P('rows')
- best_gain: float32 [32, 4, 128], P(None, 'rep', 'rows')
- node_best: float32 [32], replicated
The draws below stay inside these ranges and needn't reach their ends.
All inputs are finite; a program needn't handle non-finite values.
Results may differ from the reference program's by a relative error of at most 0.0003.
Values sent between devices are 32-bit elements; how exact they have to be, the bound alone decides.
A program may use at most 64 MiB of HBM per device.

```python
import math
import jax
import jax.numpy as jnp

F = 1024
BINS = 128
ELECT = 512
NODES = 32
PARENTS = 16
ROWS = 8192
N_REP = 4


def plant(result, key, least, largest):
    longest = result.shape.index(max(result.shape))
    spots = []
    for shift in (0, 1):
        where = [jax.random.randint(jax.random.fold_in(key, axis), (), 0, length) for axis, length in enumerate(result.shape)]
        where[longest] = (where[longest] + shift) % result.shape[longest]
        spots.append(tuple(where))
    return result.at[spots[0]].set(least).at[spots[1]].set(largest)


def level_of(rng, shape, cuts, least, high):
    def one(axis_at, blocks):
        steps = jax.random.uniform(jax.random.fold_in(jax.random.fold_in(rng, 6), axis_at), (blocks,), jnp.float32, least / len(cuts), high / len(cuts))
        return jnp.repeat(jnp.exp(steps), shape[axis_at] // blocks).reshape((-1,) + (1,) * (len(shape) - axis_at - 1))

    level = one(*cuts[0])
    for cut in cuts[1:]:
        level = level * one(*cut)
    return level


def centred(own_key, extent, deviation, bound, pieces=(), kind=jnp.bfloat16):
    loudness = level_of(own_key, extent, pieces, -0.22, 0.18) if pieces else 1.0
    drawn = jax.random.normal(own_key, extent, jnp.float32) * deviation * loudness
    return jnp.minimum(jnp.maximum(drawn, -bound), bound).astype(kind)


def setup_inputs(seed: int = 0) -> dict:
    seeds = jax.random.split(jax.random.key(seed), 8)
    return {
        "binned": plant(jax.random.randint(seeds[0], (ROWS, F), 0, BINS), jax.random.fold_in(seeds[0], 1), 0, BINS - 1).astype(jnp.int32),
        "gradients": centred(seeds[1], (ROWS,), 0.5, 3.0, ((0, 8),)),
        "hessians": jnp.clip(jnp.exp(math.log(0.25) - 2.5308688 * jax.random.uniform(seeds[2], (ROWS,), jnp.float32) ** level_of(seeds[2], (ROWS,), ((0, 8),), -0.2, 0.2)), 0.019897461, 0.25).astype(jnp.bfloat16),
        "parents": plant(jax.random.randint(seeds[3], (ROWS,), 0, PARENTS), jax.random.fold_in(seeds[3], 1), 0, PARENTS - 1).astype(jnp.int32),
        "split_feature": plant(jax.random.randint(seeds[4], (PARENTS,), 0, F), jax.random.fold_in(seeds[4], 1), 0, F - 1).astype(jnp.int32),
        "split_bin": plant(jax.random.randint(seeds[5], (PARENTS,), BINS // 4, 3 * BINS // 4), jax.random.fold_in(seeds[5], 1), BINS // 4, (3 * BINS // 4) - 1).astype(jnp.int32),
        "elected": plant(jax.random.randint(seeds[6], (NODES, ELECT), 0, F // N_REP), jax.random.fold_in(seeds[6], 1), 0, (F // N_REP) - 1).astype(jnp.int32),
    }


l2_penalty = 1.0


def reference(binned, gradients, hessians, parents, split_feature, split_bin, elected):
    row_feature = split_feature[parents]
    row_value = jnp.take_along_axis(binned, row_feature[:, None], axis=1)[:, 0]
    side_bits = (row_value > split_bin[parents]).astype(jnp.int32)
    new_nodes = (2 * parents + side_bits).astype(jnp.int32)
    slot_ids = jnp.arange(ELECT, dtype=jnp.int32)
    block_start = (slot_ids // (ELECT // N_REP)) * (F // N_REP)
    feature = (elected + block_start[None, :]).astype(jnp.int32)
    row_features = feature[new_nodes]
    row_bins = jnp.take_along_axis(binned, row_features, axis=1)
    segment = (new_nodes[:, None] * ELECT + slot_ids[None, :]) * BINS + row_bins
    segment = segment.astype(jnp.int32).reshape(-1)
    grad_wide = gradients.astype(jnp.float32)
    hess_wide = hessians.astype(jnp.float32)
    count = NODES * ELECT * BINS
    hist_grad = jax.ops.segment_sum(jnp.broadcast_to(grad_wide[:, None], row_bins.shape).reshape(-1), segment, num_segments=count).reshape(NODES, ELECT, BINS)
    hist_hess = jax.ops.segment_sum(jnp.broadcast_to(hess_wide[:, None], row_bins.shape).reshape(-1), segment, num_segments=count).reshape(NODES, ELECT, BINS)
    total_grad = jax.ops.segment_sum(grad_wide, new_nodes, num_segments=NODES)[:, None, None]
    total_hess = jax.ops.segment_sum(hess_wide, new_nodes, num_segments=NODES)[:, None, None]
    left_grad = jnp.cumsum(hist_grad, axis=2)[:, :, :-1]
    left_hess = jnp.cumsum(hist_hess, axis=2)[:, :, :-1]
    split_gain = 0.5 * (left_grad * left_grad / (left_hess + l2_penalty)
                        + (total_grad - left_grad) ** 2 / (total_hess - left_hess + l2_penalty)
                        - total_grad * total_grad / (total_hess + l2_penalty))
    best_slot = jnp.max(split_gain, axis=2)
    best_gain = best_slot.reshape(NODES, N_REP, ELECT // N_REP)
    node_best = jnp.max(best_slot, axis=1)
    return new_nodes, best_gain, node_best
```

```python
import functools

import jax
import jax.numpy as jnp
from jax import lax
from jax.experimental import pallas as pl
from jax.experimental.pallas import tpu as pltpu
from jax.sharding import PartitionSpec as P

BINS = 128
LANES = 128
MESH = pl.DeviceIdType.MESH

l2_penalty = 1.0


def partner_of(n_rows, me, d):
    if n_rows & (n_rows - 1):
        return lax.rem(me + d, n_rows) if d else me
    other = me
    for bit in range(n_rows.bit_length()):
        if d >> bit & 1:
            other = other + (1 - 2 * lax.rem(me // 2**bit, 2)) * 2**bit
    return other


def kernel(
    n_rows, n_rep, issue, arrive,
    split_feature_in, split_bin_in, binned_in, gradients_in, hessians_in, parents_in, elected_in,
    new_nodes, best_out, node_best,
    split_feature, split_bin, binned, gradients, hessians, parents, elected, in_sems, gh, left_bins, right_bins,
    side_snd, side_rcv, bins_snd, bins_rcv, node_rcv, gh_rcv, top_snd, top_rcv,
    side_ss, side_rs, gh_ss, gh_rs, node_ss, node_rs, bins_ss, bins_rs, top_ss, top_rs,
    le, acc,
):
    rows_here, block_width = binned.shape
    node_count, slots_here = elected.shape
    parent_count = split_feature.shape[0]
    owned = slots_here // n_rows
    me = lax.axis_index("rows")
    rep = lax.axis_index("rep")
    slot_of = {d: s for s, d in enumerate(arrive, 1)}

    def at(d, e):
        return (partner_of(n_rows, me, d), lax.rem(rep + e, n_rep))

    def send(src, dst, ss, rs, device):
        copy = pltpu.make_async_remote_copy(
            src_ref=src, dst_ref=dst, send_sem=ss, recv_sem=rs, device_id=device, device_id_type=MESH
        )
        copy.start()
        return copy

    with jax.named_scope("load"):
        barrier = pltpu.get_barrier_semaphore()
        greeted = [(0, e) for e in range(1, n_rep)] + [(d, 0) for d in issue]
        for d, e in greeted:
            pl.semaphore_signal(barrier, inc=1, device_id=at(d, e), device_id_type=MESH)

        loads = []
        for i, (src, dst) in enumerate(
            (
                (binned_in, binned), (split_feature_in, split_feature), (split_bin_in, split_bin), (parents_in, parents),
                (elected_in, elected), (gradients_in, gradients), (hessians_in, hessians),
            )
        ):
            loads.append(pltpu.make_async_copy(src, dst, in_sems.at[i]))
            loads[-1].start()
        for load in loads:
            load.wait()
        gh[0:1] = gradients[...].astype(jnp.float32).reshape(1, rows_here)
        gh[1:2] = hessians[...].astype(jnp.float32).reshape(1, rows_here)

    with jax.named_scope("side"):
        parent_sub = lax.broadcasted_iota(jnp.int32, (parent_count, block_width), 0)
        column = lax.broadcasted_iota(jnp.int32, (parent_count, block_width), 1) + rep * block_width
        feature_of = jnp.zeros((parent_count, block_width), jnp.int32)
        parent_row = lax.broadcasted_iota(jnp.int32, (parent_count, rows_here), 0)
        bin_of = jnp.zeros((parent_count, rows_here), jnp.int32)
        owns = jnp.zeros((parent_count, rows_here), jnp.int32)
        low = rep * block_width
        for p in range(parent_count):
            feature = split_feature[p]
            owned_here = jnp.where((feature >= low) & (feature < low + block_width), 1, 0)
            feature_of = jnp.where(parent_sub == p, feature, feature_of)
            bin_of = jnp.where(parent_row == p, split_bin[p], bin_of)
            owns = jnp.where(parent_row == p, owned_here, owns)
        picks = jnp.where(feature_of == column, 1.0, 0.0).astype(jnp.bfloat16)
        values = lax.dot_general(
            picks,
            binned[...].astype(jnp.float32).astype(jnp.bfloat16),
            (((1,), (1,)), ((), ())),
            preferred_element_type=jnp.float32,
        )
        own_parents = parents[...]
        goes = (parent_row == own_parents) & (owns > 0) & (values > bin_of.astype(jnp.float32))
        side = jnp.sum(jnp.where(goes, 1.0, 0.0), axis=0, keepdims=True)
        side_snd[...] = side

    with jax.named_scope("barwait"):
        pl.semaphore_wait(barrier, len(greeted))
        sides = []
        for e in range(1, n_rep):
            sides.append(send(side_snd, side_rcv.at[e], side_ss.at[e], side_rs.at[e], at(0, e)))
        ghs = []
        for d in issue:
            ghs.append(send(gh, gh_rcv.at[slot_of[d]], gh_ss.at[slot_of[d]], gh_rs.at[slot_of[d]], at(d, 0)))
        gh_rcv[0] = gh[...]

    with jax.named_scope("gather"):
        node_sub = lax.broadcasted_iota(jnp.int32, (node_count, rows_here), 0)
        elected_wide = elected[...].astype(jnp.float32).astype(jnp.bfloat16)
        for child, turned in ((0, left_bins), (1, right_bins)):
            child_hot = jnp.where(node_sub == 2 * own_parents + child, 1.0, 0.0).astype(jnp.bfloat16)
            index = lax.dot_general(
                child_hot, elected_wide, (((0,), (0,)), ((), ())), preferred_element_type=jnp.float32
            ).astype(jnp.int32)
            lane = index % LANES
            part = index // LANES
            chosen = None
            for start in range(block_width // LANES):
                piece = binned[:, start * LANES : (start + 1) * LANES]
                found = jnp.take_along_axis(piece, lane, axis=1, mode="promise_in_bounds")
                chosen = found if chosen is None else jnp.where(part == start, found, chosen)
            turned[...] = chosen.astype(jnp.float32).T

    with jax.named_scope("sidex"):
        for e, copy in enumerate(sides, 1):
            copy.wait()
            side = side + side_rcv[e]
        nodes = 2 * own_parents + side.astype(jnp.int32)
        new_nodes[...] = nodes
        node_rcv[0] = nodes

    with jax.named_scope("select"):
        for j in range(n_rows):
            slots = slice(j * owned, (j + 1) * owned)
            bins_snd[j] = jnp.where(side > 0.5, right_bins[slots, :], left_bins[slots, :])
        for d in issue:
            s = slot_of[d]
            send(node_rcv.at[0], node_rcv.at[s], node_ss.at[s], node_rs.at[s], at(d, 0))
            send(bins_snd.at[partner_of(n_rows, me, d)], bins_rcv.at[s], bins_ss.at[s], bins_rs.at[s], at(d, 0))
        bins_rcv[0] = bins_snd[me]

    def wait_for(s):
        for src, dst, ss, rs in (
            (gh, gh_rcv, gh_ss, gh_rs),
            (node_rcv.at[0], node_rcv, node_ss, node_rs),
            (bins_snd.at[0], bins_rcv, bins_ss, bins_rs),
        ):
            pltpu.make_async_remote_copy(
                src_ref=src, dst_ref=dst.at[s], send_sem=ss.at[s], recv_sem=rs.at[s],
                device_id=at(1, 0), device_id_type=MESH,
            ).wait()

    bin_sub = lax.broadcasted_iota(jnp.int32, (BINS, rows_here), 0).astype(jnp.float32).astype(jnp.bfloat16)
    one = jnp.ones((), jnp.bfloat16)
    none = jnp.zeros((), jnp.bfloat16)

    def add_source(s):
        there = node_sub == node_rcv[s]
        weights = jnp.concatenate(
            [jnp.where(there, gh_rcv[s, 0:1], 0.0), jnp.where(there, gh_rcv[s, 1:2], 0.0)], axis=0
        ).astype(jnp.bfloat16)
        bins = bins_rcv[s].astype(jnp.bfloat16)
        for k in range(owned):
            le[k * BINS : (k + 1) * BINS, :] = jnp.where(bins[k : k + 1] <= bin_sub, one, none).astype(le.dtype)
        return lax.dot_general(weights, le[...], (((1,), (1,)), ((), ())), preferred_element_type=jnp.float32)

    with jax.named_scope("src0"):
        acc[...] = add_source(0)

    with jax.named_scope("loop"):
        @pl.loop(1, n_rows)
        def _(s):
            with jax.named_scope("w"):
                wait_for(s)
            acc[...] += add_source(s)

    with jax.named_scope("gain"):
        lane = lax.broadcasted_iota(jnp.int32, (node_count, LANES), 1)
        total_grad = total_hess = base = None
        tops = jnp.full((node_count, LANES), -jnp.inf, jnp.float32)
        for k in range(owned):
                cols = slice(k * BINS, (k + 1) * BINS)
                left_grad = acc[0:node_count, cols]
                left_hess = acc[node_count : 2 * node_count, cols]
                if total_grad is None:
                    total_grad = jnp.broadcast_to(left_grad[:, BINS - 1 : BINS], left_grad.shape)
                    total_hess = jnp.broadcast_to(left_hess[:, BINS - 1 : BINS], left_hess.shape)
                    base = total_grad * total_grad / (total_hess + l2_penalty)
                right_grad = total_grad - left_grad
                gain = 0.5 * (
                    left_grad * left_grad / (left_hess + l2_penalty)
                    + right_grad * right_grad / (total_hess - left_hess + l2_penalty)
                    - base
                )
                top = jnp.max(jnp.where(lane < BINS - 1, gain, -jnp.inf), axis=1, keepdims=True)
                tops = jnp.where(lane == k, top, tops)
        turned = tops.T
        best_out[...] = turned[0:owned]
        best = jnp.max(turned[0:owned], axis=0, keepdims=True)
        top_snd[...] = best

    with jax.named_scope("top"):
        others = [(d, e) for d in (*issue, 0) for e in range(n_rep) if d or e]
        sent = []
        for i, (d, e) in enumerate(others):
            sent.append(send(top_snd, top_rcv.at[i], top_ss.at[i], top_rs.at[i], at(d, e)))
        for i, copy in enumerate(sent):
            copy.wait()
            best = jnp.maximum(best, top_rcv[i])
        node_best[...] = best


def hand_on(*refs):
    for src, dst in zip(refs[:3], refs[3:]):
        dst[...] = src[...]


def body(n_rows, n_rep, binned, gradients, hessians, parents, split_feature, split_bin, elected):
    rows_here, block_width = binned.shape
    node_count, slots_here = elected.shape
    owned = slots_here // n_rows
    f32 = jnp.float32
    vmem = pl.BlockSpec(memory_space=pltpu.VMEM)
    dma = pltpu.SemaphoreType.DMA
    order = tuple(range(1, n_rows))
    args = (split_feature, split_bin, binned, gradients, hessians, parents.reshape(1, rows_here), elected)
    made = pl.pallas_call(
        functools.partial(kernel, n_rows, n_rep, order, order),
        out_shape=(
            jax.ShapeDtypeStruct((1, rows_here), jnp.int32),
            jax.ShapeDtypeStruct((owned, node_count), f32),
            jax.ShapeDtypeStruct((1, node_count), f32),
        ),
        in_specs=[pl.BlockSpec(memory_space=pltpu.HBM)] * 7,
        out_specs=(vmem, vmem, vmem),
        scratch_shapes=[
            pltpu.SMEM(split_feature.shape, jnp.int32),
            pltpu.SMEM(split_bin.shape, jnp.int32),
            pltpu.VMEM(binned.shape, jnp.int32),
            pltpu.VMEM(gradients.shape, gradients.dtype),
            pltpu.VMEM(hessians.shape, hessians.dtype),
            pltpu.VMEM((1, rows_here), jnp.int32),
            pltpu.VMEM(elected.shape, jnp.int32),
            dma((7,)),
            pltpu.VMEM((2, rows_here), f32),
            pltpu.VMEM((slots_here, rows_here), f32),
            pltpu.VMEM((slots_here, rows_here), f32),
            pltpu.VMEM((1, rows_here), f32),
            pltpu.VMEM((n_rep, 1, rows_here), f32),
            pltpu.VMEM((n_rows, owned, rows_here), f32),
            pltpu.VMEM((n_rows, owned, rows_here), f32),
            pltpu.VMEM((n_rows, 1, rows_here), jnp.int32),
            pltpu.VMEM((n_rows, 2, rows_here), f32),
            pltpu.VMEM((1, node_count), f32),
            pltpu.VMEM((n_rows * n_rep - 1, 1, node_count), f32),
        ]
        + [dma((n_rep,))] * 2 + [dma((n_rows,))] * 6 + [dma((n_rows * n_rep - 1,))] * 2
        + [pltpu.VMEM((owned * BINS, rows_here), jnp.float8_e4m3fn), pltpu.VMEM((2 * node_count, owned * BINS), f32)],
        compiler_params=pltpu.CompilerParams(collective_id=0, has_side_effects=True, vmem_limit_bytes=16 * 2**20),
    )(*(pltpu.with_memory_space_constraint(a, pltpu.HBM) for a in args))
    new_nodes, best, node_best = pl.pallas_call(
        hand_on,
        out_shape=tuple(jax.ShapeDtypeStruct(a.shape, a.dtype) for a in made),
        in_specs=[vmem] * 3,
        out_specs=(vmem,) * 3,
        compiler_params=pltpu.CompilerParams(vmem_limit_bytes=2**20),
    )(*made)
    return (
        new_nodes.reshape(rows_here),
        best.T.reshape(node_count, 1, owned),
        node_best.reshape(node_count),
    )


def solution(mesh):
    return jax.shard_map(
        functools.partial(body, mesh.shape["rows"], mesh.shape["rep"]),
        mesh=mesh,
        in_specs=(P("rows", "rep"), P("rows"), P("rows"), P("rows"), P(), P(), P(None, "rep")),
        out_specs=(P("rows"), P(None, "rep", "rows"), P()),
        check_vma=False,
    )
```

```python
import functools

import jax
import jax.numpy as jnp
from jax import lax
from jax.experimental import pallas as pl
from jax.experimental.pallas import tpu as pltpu
from jax.sharding import PartitionSpec as P

BINS = 128
LANES = 128
MESH = pl.DeviceIdType.MESH

l2_penalty = 1.0


def partner_of(n_rows, me, d):
    if n_rows & (n_rows - 1):
        return lax.rem(me + d, n_rows) if d else me
    other = me
    for bit in range(n_rows.bit_length()):
        if d >> bit & 1:
            other = other + (1 - 2 * lax.rem(me // 2**bit, 2)) * 2**bit
    return other


def kernel(
    n_rows, n_rep, issue, arrive,
    split_feature_in, split_bin_in, binned_in, gradients_in, hessians_in, parents_in, elected_in,
    new_nodes, best_out, node_best,
    split_feature, split_bin, binned, gradients, hessians, parents, elected, both_bins,
    side_snd, side_rcv, bins_snd, bins_rcv, early, own_gh, weights, le, acc, top_snd, top_rcv,
    in_sems, side_ss, side_rs, early_ss, early_rs, fan_ss, fan_rs, bins_ss, bins_rs, top_ss, top_rs,
):
    rows_here, block_width = binned.shape
    node_count, slots_here = elected.shape
    parent_count = split_feature.shape[0]
    owned = slots_here // n_rows
    part_rows = rows_here // n_rep
    me = lax.axis_index("rows")
    rep = lax.axis_index("rep")
    slot_of = {d: s for s, d in enumerate(arrive, 1)}
    pieces = 2 if owned % 16 == 0 else 1
    share = owned // pieces

    def at(d, e):
        return (partner_of(n_rows, me, d), lax.rem(rep + e, n_rep))

    def remote(src, dst, ss, rs, device):
        return pltpu.make_async_remote_copy(
            src_ref=src, dst_ref=dst, send_sem=ss, recv_sem=rs, device_id=device, device_id_type=MESH
        )

    def all_of(ref, ss, rs):
        return remote(ref, ref, ss, rs, at(1, 0))

    with jax.named_scope("load"):
        barrier = pltpu.get_barrier_semaphore()
        greeted = [(0, e) for e in range(1, n_rep)] + [(d, 0) for d in issue]
        for d, e in greeted:
            pl.semaphore_signal(barrier, inc=1, device_id=at(d, e), device_id_type=MESH)

        loads = []
        quarter = rows_here // 4
        for i, (src, dst) in enumerate(
            (
                (split_feature_in, split_feature), (split_bin_in, split_bin), (parents_in, parents),
                *((binned_in.at[c * quarter : (c + 1) * quarter], binned.at[c * quarter : (c + 1) * quarter]) for c in range(4)),
                (gradients_in, gradients), (hessians_in, hessians), (elected_in, elected),
            )
        ):
            loads.append(pltpu.make_async_copy(src, dst, in_sems.at[i]))
            loads[-1].start()
        for load in loads[:3]:
            load.wait()

    with jax.named_scope("side"):
        parent_sub = lax.broadcasted_iota(jnp.int32, (parent_count, block_width), 0)
        column = lax.broadcasted_iota(jnp.int32, (parent_count, block_width), 1) + rep * block_width
        feature_of = jnp.zeros((parent_count, block_width), jnp.int32)
        parent_row = lax.broadcasted_iota(jnp.int32, (parent_count, rows_here), 0)
        bin_of = jnp.zeros((parent_count, rows_here), jnp.int32)
        owns = jnp.zeros((parent_count, rows_here), jnp.int32)
        low = rep * block_width
        for p in range(parent_count):
            feature = split_feature[p]
            owned_here = jnp.where((feature >= low) & (feature < low + block_width), 1, 0)
            feature_of = jnp.where(parent_sub == p, feature, feature_of)
            bin_of = jnp.where(parent_row == p, split_bin[p], bin_of)
            owns = jnp.where(parent_row == p, owned_here, owns)
        for load in loads[3:7]:
            load.wait()
        picks = jnp.where(feature_of == column, 1.0, 0.0).astype(jnp.bfloat16)
        values = lax.dot_general(
            picks,
            binned[...].astype(jnp.float32).astype(jnp.bfloat16),
            (((1,), (1,)), ((), ())),
            preferred_element_type=jnp.float32,
        )
        own_parents = parents[...]
        goes = (parent_row == own_parents) & (owns > 0) & (values > bin_of.astype(jnp.float32))
        side = jnp.sum(jnp.where(goes, 1.0, 0.0), axis=0, keepdims=True)
        side_snd[...] = side
        for load in loads[7:9]:
            load.wait()
        own_gh[0:1] = gradients[...].astype(jnp.float32).reshape(1, rows_here)
        own_gh[1:2] = hessians[...].astype(jnp.float32).reshape(1, rows_here)
        mine = pl.ds(pl.multiple_of(rep * part_rows, part_rows), part_rows)
        for f in range(n_rep):
            early[0, 0, f : f + 1] = side[:, f * part_rows : (f + 1) * part_rows]
        early[0, 0, n_rep : n_rep + 2] = own_gh[:, mine]
        early[0, 0, n_rep + 2 : n_rep + 3] = parents[:, mine].astype(jnp.float32)
        early[0, 0, n_rep + 3 :] = jnp.zeros((early.shape[2] - n_rep - 3, part_rows), jnp.float32)

    with jax.named_scope("barwait"):
        pl.semaphore_wait(barrier, len(greeted))
        for e in range(1, n_rep):
            remote(side_snd, side_rcv.at[e - 1], side_ss, side_rs, at(0, e)).start()
        for d in issue:
            remote(early.at[0, 0], early.at[0, slot_of[d]], early_ss, early_rs, at(d, 0)).start()

    with jax.named_scope("gather"):
        loads[9].wait()
        elected_wide = elected[...].astype(jnp.float32).astype(jnp.bfloat16)
        tile = rows_here // 2
        node_tile = lax.broadcasted_iota(jnp.int32, (node_count, tile), 0)

        @pl.loop(0, rows_here // tile)
        def _(t):
            here = pl.ds(pl.multiple_of(t * tile, tile), tile)
            above = 2 * parents[:, here]
            packed = None
            for child in range(2):
                child_hot = jnp.where(node_tile == above + child, 1.0, 0.0).astype(jnp.bfloat16)
                index = lax.dot_general(
                    child_hot, elected_wide, (((0,), (0,)), ((), ())), preferred_element_type=jnp.float32
                ).astype(jnp.int32)
                lane = index & (LANES - 1)
                part = lax.shift_right_logical(index, LANES.bit_length() - 1)
                chosen = None
                for start in range(block_width // LANES):
                    piece = binned[here, start * LANES : (start + 1) * LANES]
                    found = jnp.take_along_axis(piece, lane, axis=1, mode="promise_in_bounds")
                    chosen = found if chosen is None else jnp.where(part == start, found, chosen)
                packed = chosen if packed is None else packed + chosen * 256
            both_bins[:, here] = packed.T

    with jax.named_scope("sidex"):
        sides = all_of(side_rcv, side_ss, side_rs)
        sides.wait_recv()
        for e in range(1, n_rep):
            side = side + side_rcv[e - 1]
        side = side.astype(jnp.int32)
        nodes = 2 * parents[...] + side
        new_nodes[...] = nodes

    with jax.named_scope("select"):
        shift = side * 8
        for j in range(n_rows):
            slots = slice(j * owned, (j + 1) * owned)
            bins_snd[j] = lax.shift_right_logical(both_bins[slots, :], jnp.broadcast_to(shift, (owned, rows_here))) & 255
        for d in issue:
            s = slot_of[d]
            for piece in range(pieces):
                some = slice(piece * share, (piece + 1) * share)
                remote(
                    bins_snd.at[partner_of(n_rows, me, d), some], bins_rcv.at[s, some],
                    bins_ss, bins_rs.at[s * pieces + piece], at(d, 0),
                ).start()
        bins_rcv[0] = bins_snd[me]

    with jax.named_scope("nodew"):
        earlies = all_of(early.at[0, 1:n_rows], early_ss, early_rs)
        earlies.wait_recv()
        for e in range(1, n_rep):
            remote(early.at[0, 1:n_rows], early.at[e, 1:n_rows], fan_ss, fan_rs, at(0, e)).start()
        fans = all_of(early.at[1:n_rep, 1:n_rows], fan_ss, fan_rs)

    bin_sub = lax.broadcasted_iota(jnp.int32, (BINS, rows_here), 0).astype(jnp.float32).astype(jnp.bfloat16)
    node_sub = lax.broadcasted_iota(jnp.int32, (node_count, rows_here), 0)
    one = jnp.ones((), jnp.bfloat16)
    none = jnp.zeros((), jnp.bfloat16)
    acc[...] = jnp.zeros_like(acc)

    def weigh(node, grad, hess):
        there = node_sub == node
        return jnp.concatenate([jnp.where(there, grad, 0.0), jnp.where(there, hess, 0.0)], axis=0).astype(jnp.bfloat16)

    weights[0] = weigh(nodes, own_gh[0:1], own_gh[1:2])

    with jax.named_scope("loop"):
        @pl.loop(0, n_rows * pieces)
        def _(t):
            s = t // pieces
            piece = t % pieces
            first = pl.multiple_of(piece * share, share)
            with jax.named_scope("w"):
                @pl.when(t == pieces)
                def _():
                    fans.wait_recv()

                    @pl.loop(1, n_rows)
                    def _(u):
                        node, grad, hess = [], [], []
                        for f in range(n_rep):
                            e = lax.rem(rep + n_rep - f, n_rep)
                            node.append(
                                2.0 * early[e, u, n_rep + 2 : n_rep + 3]
                                + sum(early[c, u, f : f + 1] for c in range(n_rep))
                            )
                            grad.append(early[e, u, n_rep : n_rep + 1])
                            hess.append(early[e, u, n_rep + 1 : n_rep + 2])
                        node, grad, hess = (jnp.concatenate(x, axis=1) for x in (node, grad, hess))
                        weights[u] = weigh(node.astype(jnp.int32), grad, hess)

                @pl.when(s > 0)
                def _():
                    all_of(bins_rcv.at[s, pl.ds(first, share)], bins_ss, bins_rs.at[t]).wait_recv()
            bins = bins_rcv[s, pl.ds(first, share), :].astype(jnp.float32).astype(jnp.bfloat16)
            for k in range(share):
                le[k * BINS : (k + 1) * BINS, :] = jnp.where(bins[k : k + 1] <= bin_sub, one, none).astype(le.dtype)
            acc[piece] += lax.dot_general(
                weights[s], le[...], (((1,), (1,)), ((), ())), preferred_element_type=jnp.float32
            )

    with jax.named_scope("gain"):
        lane = lax.broadcasted_iota(jnp.int32, (node_count, LANES), 1)
        total_grad = total_hess = base = None
        tops = jnp.full((node_count, LANES), -jnp.inf, jnp.float32)
        for k in range(owned):
                cols = slice(k % share * BINS, (k % share + 1) * BINS)
                left_grad = acc[k // share, 0:node_count, cols]
                left_hess = acc[k // share, node_count : 2 * node_count, cols]
                if total_grad is None:
                    total_grad = jnp.broadcast_to(left_grad[:, BINS - 1 : BINS], left_grad.shape)
                    total_hess = jnp.broadcast_to(left_hess[:, BINS - 1 : BINS], left_hess.shape)
                    base = total_grad * total_grad / (total_hess + l2_penalty)
                right_grad = total_grad - left_grad
                gain = 0.5 * (
                    left_grad * left_grad / (left_hess + l2_penalty)
                    + right_grad * right_grad / (total_hess - left_hess + l2_penalty)
                    - base
                )
                top = jnp.max(jnp.where(lane < BINS - 1, gain, -jnp.inf), axis=1, keepdims=True)
                tops = jnp.where(lane == k, top, tops)
        turned = tops.T
        best_out[...] = turned[0:owned]
        best = jnp.max(turned[0:owned], axis=0, keepdims=True)
        top_snd[...] = best

    with jax.named_scope("top"):
        others = [(d, e) for d in (*issue, 0) for e in range(n_rep) if d or e]
        for i, (d, e) in enumerate(others):
            remote(top_snd, top_rcv.at[i], top_ss, top_rs, at(d, e)).start()
        tops_all = all_of(top_rcv, top_ss, top_rs)
        tops_all.wait_recv()
        for i in range(len(others)):
            best = jnp.maximum(best, top_rcv[i])
        node_best[...] = best
        for sent in (sides, earlies, fans, all_of(bins_rcv.at[1:n_rows], bins_ss, bins_rs.at[0]), tops_all):
            sent.wait_send()


def hand_on(*refs):
    for src, dst in zip(refs[:3], refs[3:]):
        dst[...] = src[...]


def body(n_rows, n_rep, binned, gradients, hessians, parents, split_feature, split_bin, elected):
    rows_here, block_width = binned.shape
    node_count, slots_here = elected.shape
    owned = slots_here // n_rows
    pieces = 2 if owned % 16 == 0 else 1
    f32 = jnp.float32
    vmem = pl.BlockSpec(memory_space=pltpu.VMEM)
    dma = pltpu.SemaphoreType.DMA
    order = tuple(range(1, n_rows))
    args = (split_feature, split_bin, binned, gradients, hessians, parents.reshape(1, rows_here), elected)
    made = pl.pallas_call(
        functools.partial(kernel, n_rows, n_rep, order, order),
        out_shape=(
            jax.ShapeDtypeStruct((1, rows_here), jnp.int32),
            jax.ShapeDtypeStruct((owned, node_count), f32),
            jax.ShapeDtypeStruct((1, node_count), f32),
        ),
        in_specs=[pl.BlockSpec(memory_space=pltpu.HBM)] * 7,
        out_specs=(vmem, vmem, vmem),
        scratch_shapes=[
            pltpu.SMEM(split_feature.shape, jnp.int32),
            pltpu.SMEM(split_bin.shape, jnp.int32),
            pltpu.VMEM(binned.shape, jnp.int32),
            pltpu.VMEM(gradients.shape, gradients.dtype),
            pltpu.VMEM(hessians.shape, hessians.dtype),
            pltpu.VMEM((1, rows_here), jnp.int32),
            pltpu.VMEM(elected.shape, jnp.int32),
            pltpu.VMEM((slots_here, rows_here), jnp.int32),
            pltpu.VMEM((1, rows_here), f32),
            pltpu.VMEM((n_rep - 1, 1, rows_here), f32),
            pltpu.VMEM((n_rows, owned, rows_here), jnp.int32),
            pltpu.VMEM((n_rows, owned, rows_here), jnp.int32),
            pltpu.VMEM((n_rep, n_rows, -(-(n_rep + 3) // 8) * 8, rows_here // n_rep), f32),
            pltpu.VMEM((2, rows_here), f32),
            pltpu.VMEM((n_rows, 2 * node_count, rows_here), jnp.bfloat16),
            pltpu.VMEM((owned // pieces * BINS, rows_here), jnp.float8_e4m3fn),
            pltpu.VMEM((pieces, 2 * node_count, owned // pieces * BINS), f32),
            pltpu.VMEM((1, node_count), f32),
            pltpu.VMEM((n_rows * n_rep - 1, 1, node_count), f32),
            dma((10,)),
        ]
        + [dma(())] * 7
        + [dma((n_rows * pieces,))]
        + [dma(())] * 2,
        compiler_params=pltpu.CompilerParams(collective_id=0, has_side_effects=True, vmem_limit_bytes=16 * 2**20),
    )(*(pltpu.with_memory_space_constraint(a, pltpu.HBM) for a in args))
    new_nodes, best, node_best = pl.pallas_call(
        hand_on,
        out_shape=tuple(jax.ShapeDtypeStruct(a.shape, a.dtype) for a in made),
        in_specs=[vmem] * 3,
        out_specs=(vmem,) * 3,
        compiler_params=pltpu.CompilerParams(vmem_limit_bytes=2**20),
    )(*made)
    return (
        new_nodes.reshape(rows_here),
        best.T.reshape(node_count, 1, owned),
        node_best.reshape(node_count),
    )


def solution(mesh):
    return jax.shard_map(
        functools.partial(body, mesh.shape["rows"], mesh.shape["rep"]),
        mesh=mesh,
        in_specs=(P("rows", "rep"), P("rows"), P("rows"), P("rows"), P(), P(), P(None, "rep")),
        out_specs=(P("rows"), P(None, "rep", "rows"), P()),
        check_vma=False,
    )
```

```python
import functools

import jax
import jax.numpy as jnp
from jax import lax
from jax.experimental import pallas as pl
from jax.experimental.pallas import tpu as pltpu
from jax.sharding import PartitionSpec as P

BINS = 128
LANES = 128
MESH = pl.DeviceIdType.MESH

l2_penalty = 1.0


def partner_of(n_rows, me, d):
    if n_rows & (n_rows - 1):
        return lax.rem(me + d, n_rows) if d else me
    other = me
    for bit in range(n_rows.bit_length()):
        if d >> bit & 1:
            other = other + (1 - 2 * lax.rem(me // 2**bit, 2)) * 2**bit
    return other


def parts_of(pieces, owned, rows_here):
    everything = slice(0, owned), slice(0, rows_here)
    if pieces == 1:
        return [everything], [[everything]]
    share = owned // pieces
    step = max(rows_here // 4, 2 * LANES)
    upper, lower = slice(0, share), slice(share, owned)
    usual = [(upper, slice(0, rows_here)), (lower, slice(LANES, rows_here))]
    last = [[(upper, slice(0, step)), (lower, slice(LANES, step))]]
    for begin in range(step, rows_here, step):
        last.append([(slice(0, owned), slice(begin, min(begin + step, rows_here)))])
    return usual, last


def kernel(
    n_rows, n_rep, pieces, issue, arrive,
    split_feature_in, split_bin_in, binned_in, gradients_in, hessians_in, parents_in, elected_in,
    new_nodes, best_out, node_best,
    split_feature, split_bin, binned, gradients, hessians, parents, elected, both_bins,
    side_snd, side_rcv, guess_snd, guess_rcv, bins_snd, bins_rcv, early, own_gh, weights, le, acc, top_snd, top_rcv,
    in_sems, side_ss, side_rs, early_ss, early_rs, fan_ss, fan_rs, guess_ss, guess_rs, bins_ss, bins_rs, top_ss, top_rs,
):
    rows_here, block_width = binned.shape
    node_count, slots_here = elected.shape
    parent_count = split_feature.shape[0]
    owned = slots_here // n_rows
    part_rows = rows_here // n_rep
    me = lax.axis_index("rows")
    rep = lax.axis_index("rep")
    slot_of = {d: s for s, d in enumerate(arrive, 1)}
    share = owned // pieces
    parts, steps = parts_of(pieces, owned, rows_here)
    ends = [part for step in steps for part in step]
    hedged = slice(owned - share, owned)
    groups = [(1, n_rows)]

    def at(d, e):
        return (partner_of(n_rows, me, d), lax.rem(rep + e, n_rep))

    def remote(src, dst, ss, rs, device):
        return pltpu.make_async_remote_copy(
            src_ref=src, dst_ref=dst, send_sem=ss, recv_sem=rs, device_id=device, device_id_type=MESH
        )

    def all_of(ref, ss, rs):
        return remote(ref, ref, ss, rs, at(1, 0))

    with jax.named_scope("load"):
        barrier = pltpu.get_barrier_semaphore()
        greeted = [(0, e) for e in range(1, n_rep)] + [(d, 0) for d in issue]
        for d, e in greeted:
            pl.semaphore_signal(barrier, inc=1, device_id=at(d, e), device_id_type=MESH)

        loads = []
        for i, (src, dst) in enumerate(
            (
                (split_feature_in, split_feature), (split_bin_in, split_bin), (parents_in, parents),
                (binned_in, binned),
                (gradients_in, gradients), (hessians_in, hessians), (elected_in, elected),
            )
        ):
            loads.append(pltpu.make_async_copy(src, dst, in_sems.at[i]))
            loads[-1].start()
        for load in loads[:3]:
            load.wait()

    with jax.named_scope("side"):
        parent_sub = lax.broadcasted_iota(jnp.int32, (parent_count, block_width), 0)
        column = lax.broadcasted_iota(jnp.int32, (parent_count, block_width), 1) + rep * block_width
        feature_of = jnp.zeros((parent_count, block_width), jnp.int32)
        parent_row = lax.broadcasted_iota(jnp.int32, (parent_count, rows_here), 0)
        bin_of = jnp.zeros((parent_count, rows_here), jnp.int32)
        owns = jnp.zeros((parent_count, rows_here), jnp.int32)
        low = rep * block_width
        for p in range(parent_count):
            feature = split_feature[p]
            owned_here = jnp.where((feature >= low) & (feature < low + block_width), 1, 0)
            feature_of = jnp.where(parent_sub == p, feature, feature_of)
            bin_of = jnp.where(parent_row == p, split_bin[p], bin_of)
            owns = jnp.where(parent_row == p, owned_here, owns)
        for load in loads[3:4]:
            load.wait()
        picks = jnp.where(feature_of == column, 1.0, 0.0).astype(jnp.bfloat16)
        values = lax.dot_general(
            picks,
            binned[...].astype(jnp.float32).astype(jnp.bfloat16),
            (((1,), (1,)), ((), ())),
            preferred_element_type=jnp.float32,
        )
        own_parents = parents[...]
        goes = (parent_row == own_parents) & (owns > 0) & (values > bin_of.astype(jnp.float32))
        side = jnp.sum(jnp.where(goes, 1.0, 0.0), axis=0, keepdims=True)
        side_snd[...] = side
        for load in loads[4:6]:
            load.wait()
        own_gh[0:1] = gradients[...].astype(jnp.float32).reshape(1, rows_here)
        own_gh[1:2] = hessians[...].astype(jnp.float32).reshape(1, rows_here)
        mine = pl.ds(pl.multiple_of(rep * part_rows, part_rows), part_rows)
        for f in range(n_rep):
            early[0, 0, f] = side[:, f * part_rows : (f + 1) * part_rows]
        early[0, 0, n_rep] = own_gh[0:1, mine]
        early[0, 0, n_rep + 1] = own_gh[1:2, mine]
        early[0, 0, n_rep + 2] = parents[:, mine].astype(jnp.float32)

    with jax.named_scope("barwait"):
        pl.semaphore_wait(barrier, len(greeted))
        for e in range(1, n_rep):
            remote(side_snd, side_rcv.at[e - 1], side_ss, side_rs, at(0, e)).start()
        for d in issue[::-1]:
            s = slot_of[d]
            g = [i for i, (low, high) in enumerate(groups) if low <= s < high][0]
            remote(early.at[0, 0], early.at[0, s], early_ss.at[g], early_rs.at[g], at(d, 0)).start()

    with jax.named_scope("gather"):
        loads[6].wait()
        elected_wide = elected[...].astype(jnp.float32).astype(jnp.bfloat16)

        def gather(begin, end):
            here = slice(begin, end)
            node_tile = lax.broadcasted_iota(jnp.int32, (node_count, end - begin), 0)
            above = 2 * own_parents[:, here]
            pieces_here = [
                binned[here, start * LANES : (start + 1) * LANES] for start in range(block_width // LANES)
            ]
            tables = [
                pieces_here[g] + (pieces_here[g + 1] * 256 if g + 1 < len(pieces_here) else 0)
                for g in range(0, len(pieces_here), 2)
            ]
            packed = None
            for child in range(2):
                child_hot = jnp.where(node_tile == above + child, 1.0, 0.0).astype(jnp.bfloat16)
                index = lax.dot_general(
                    child_hot, elected_wide, (((0,), (0,)), ((), ())), preferred_element_type=jnp.float32
                ).astype(jnp.int32)
                lane = index & (LANES - 1)
                part = lax.shift_right_logical(index, LANES.bit_length() - 1)
                chosen = None
                for g, table in enumerate(tables):
                    found = jnp.take_along_axis(table, lane, axis=1, mode="promise_in_bounds")
                    found = lax.shift_right_logical(found, (part & 1) * 8) & 255
                    chosen = found if chosen is None else jnp.where(part // 2 == g, found, chosen)
                packed = chosen if packed is None else packed + chosen * 256
            both_bins[:, here] = packed.T

        gather(0, LANES)
        if pieces > 1:
            for j in range(n_rows):
                two = both_bins[j * owned + owned - share : (j + 1) * owned, 0:LANES]
                guess_snd[j, 0] = two & 255
                guess_snd[j, 1] = lax.shift_right_logical(two, 8)
            for d in issue:
                remote(
                    guess_snd.at[partner_of(n_rows, me, d)], guess_rcv.at[slot_of[d]], guess_ss, guess_rs, at(d, 0)
                ).start()
        gather(LANES, rows_here)

    with jax.named_scope("sidex"):
        sides = all_of(side_rcv, side_ss, side_rs)
        sides.wait_recv()
        for e in range(1, n_rep):
            side = side + side_rcv[e - 1]
        side = side.astype(jnp.int32)
        nodes = 2 * parents[...] + side
        new_nodes[...] = nodes

    with jax.named_scope("select"):
        shift = side * 8
        for j in range(n_rows):
            slots = slice(j * owned, (j + 1) * owned)
            bins_snd[j] = lax.shift_right_logical(both_bins[slots, :], jnp.broadcast_to(shift, (owned, rows_here))) & 255
        for d in issue:
            s = slot_of[d]
            for i, (slots, rows) in enumerate(ends if s == n_rows - 1 else parts):
                remote(
                    bins_snd.at[partner_of(n_rows, me, d), slots, rows], bins_rcv.at[s, slots, rows],
                    bins_ss.at[i + (len(parts) if s == n_rows - 1 else 0)], bins_rs.at[(s - 1) * len(parts) + i], at(d, 0),
                ).start()
        bins_rcv[0] = bins_snd[me]

    def early_of(g):
        return all_of(early.at[0, groups[g][0] : groups[g][1]], early_ss.at[g], early_rs.at[g])

    def fan_of(g):
        return all_of(early.at[1:n_rep, groups[g][0] : groups[g][1]], fan_ss.at[g], fan_rs.at[g])

    def fan(g):
        early_of(g).wait_recv()
        some = slice(*groups[g])
        for e in range(1, n_rep):
            remote(early.at[0, some], early.at[e, some], fan_ss.at[g], fan_rs.at[g], at(0, e)).start()

    with jax.named_scope("nodew"):
        fan(0)

    bin_sub = lax.broadcasted_iota(jnp.int32, (BINS, rows_here), 0).astype(jnp.float32).astype(jnp.bfloat16)
    node_sub = lax.broadcasted_iota(jnp.int32, (node_count, rows_here), 0)
    one = jnp.ones((), jnp.bfloat16)
    none = jnp.zeros((), jnp.bfloat16)
    acc[...] = jnp.zeros_like(acc)

    def weigh(node, grad, hess):
        there = node_sub == node
        return jnp.concatenate([jnp.where(there, grad, 0.0), jnp.where(there, hess, 0.0)], axis=0).astype(jnp.bfloat16)

    weights[0] = weigh(nodes, own_gh[0:1], own_gh[1:2])

    def arrived(s, i):
        slots, rows = parts[i]
        all_of(bins_rcv.at[s, slots, rows], bins_ss.at[i], bins_rs.at[(s - 1) * len(parts) + i]).wait_recv()

    def ended(i):
        slots, rows = ends[i]
        return all_of(
            bins_rcv.at[n_rows - 1, slots, rows], bins_ss.at[len(parts) + i], bins_rs.at[(n_rows - 2) * len(parts) + i]
        )

    def add(s, slots, rows):
        bins = bins_rcv[s, slots, rows].astype(jnp.float32).astype(jnp.bfloat16)
        cols = slice(slots.start * BINS, slots.stop * BINS)
        for k in range(slots.stop - slots.start):
            at_k = slice((slots.start + k) * BINS, (slots.start + k + 1) * BINS)
            le[at_k, rows] = jnp.where(bins[k : k + 1] <= bin_sub[:, rows], one, none).astype(le.dtype)
        acc[:, cols] += lax.dot_general(
            weights[s, :, rows], le[cols, rows], (((1,), (1,)), ((), ())), preferred_element_type=jnp.float32
        )

    guesses = all_of(guess_rcv.at[1:n_rows], guess_ss, guess_rs) if pieces > 1 else None

    def fill(g):
        fan_of(g).wait_recv()

        @pl.loop(*groups[g])
        def _(u):
            above, right, grad, hess = [], [], [], []
            for f in range(n_rep):
                e = lax.rem(rep + n_rep - f, n_rep)
                above.append(early[e, u, n_rep + 2])
                right.append(sum(early[c, u, f] for c in range(n_rep)))
                grad.append(early[e, u, n_rep])
                hess.append(early[e, u, n_rep + 1])
            above, right, grad, hess = (jnp.concatenate(x, axis=1) for x in (above, right, grad, hess))
            weights[u] = weigh((2.0 * above + right).astype(jnp.int32), grad, hess)
            if pieces > 1:
                bins_rcv[u, hedged, 0:LANES] = jnp.where(right[:, 0:LANES] > 0.5, guess_rcv[u, 1], guess_rcv[u, 0])

    everything = slice(0, rows_here)
    with jax.named_scope("own"):
        for piece in range(pieces):
            add(0, slice(piece * share, (piece + 1) * share), everything)
        for g in range(1, len(groups)):
            fan(g)
        if pieces > 1:
            guesses.wait_recv()
    with jax.named_scope("fill"):
        fill(0)

    with jax.named_scope("loop"):
        @pl.loop(1, n_rows - 1)
        def _(s):
            for piece in range(pieces):
                with jax.named_scope("w"):
                    arrived(s, piece)
                add(s, slice(piece * share, (piece + 1) * share), everything)

    i = 0
    for step in steps:
        with jax.named_scope("last"):
            with jax.named_scope("lw"):
                for _ in step:
                    ended(i).wait_recv()
                    i += 1
            add(n_rows - 1, slice(0, owned), slice(0 if step is steps[0] else step[0][1].start, step[0][1].stop))

    lane = lax.broadcasted_iota(jnp.int32, (node_count, LANES), 1)
    tops = jnp.full((node_count, LANES), -jnp.inf, jnp.float32)
    total_grad = total_hess = base = None
    for piece in range(pieces):
        with jax.named_scope("gain"):
            for k in range(share):
                cols = slice((piece * share + k) * BINS, (piece * share + k + 1) * BINS)
                left_grad = acc[0:node_count, cols]
                left_hess = acc[node_count : 2 * node_count, cols]
                if total_grad is None:
                    total_grad = jnp.broadcast_to(left_grad[:, BINS - 1 : BINS], left_grad.shape)
                    total_hess = jnp.broadcast_to(left_hess[:, BINS - 1 : BINS], left_hess.shape)
                    base = total_grad * total_grad / (total_hess + l2_penalty)
                right_grad = total_grad - left_grad
                gain = 0.5 * (
                    left_grad * left_grad / (left_hess + l2_penalty)
                    + right_grad * right_grad / (total_hess - left_hess + l2_penalty)
                    - base
                )
                top = jnp.max(jnp.where(lane < BINS - 1, gain, -jnp.inf), axis=1, keepdims=True)
                tops = jnp.where(lane == piece * share + k, top, tops)
    turned = tops.T
    best_out[...] = turned[0:owned]
    best = jnp.max(turned[0:owned], axis=0, keepdims=True)
    top_snd[...] = best

    with jax.named_scope("top"):
        others = [(d, e) for d in (*issue, 0) for e in range(n_rep) if d or e]
        for i, (d, e) in enumerate(others):
            remote(top_snd, top_rcv.at[i], top_ss, top_rs, at(d, e)).start()
        tops_all = all_of(top_rcv, top_ss, top_rs)
        tops_all.wait_recv()
        for i in range(len(others)):
            best = jnp.maximum(best, top_rcv[i])
        node_best[...] = best
        for sent in (sides, tops_all, *map(early_of, range(len(groups))), *map(fan_of, range(len(groups)))):
            sent.wait_send()
        if pieces > 1:
            guesses.wait_send()
        if n_rows > 2:
            for i, (slots, rows) in enumerate(parts):
                all_of(bins_rcv.at[1 : n_rows - 1, slots, rows], bins_ss.at[i], bins_rs.at[0]).wait_send()
        for i in range(len(ends)):
            ended(i).wait_send()


def hand_on(*refs):
    for src, dst in zip(refs[:3], refs[3:]):
        dst[...] = src[...]


def body(n_rows, n_rep, binned, gradients, hessians, parents, split_feature, split_bin, elected):
    rows_here, block_width = binned.shape
    node_count, slots_here = elected.shape
    owned = slots_here // n_rows
    pieces = 2 if owned % 16 == 0 and rows_here > 2 * LANES else 1
    parts, steps = parts_of(pieces, owned, rows_here)
    parts, ends = len(parts), sum(map(len, steps))
    f32 = jnp.float32
    vmem = pl.BlockSpec(memory_space=pltpu.VMEM)
    dma = pltpu.SemaphoreType.DMA
    order = tuple(range(1, n_rows))
    args = (split_feature, split_bin, binned, gradients, hessians, parents.reshape(1, rows_here), elected)
    made = pl.pallas_call(
        functools.partial(kernel, n_rows, n_rep, pieces, order, order),
        out_shape=(
            jax.ShapeDtypeStruct((1, rows_here), jnp.int32),
            jax.ShapeDtypeStruct((owned, node_count), f32),
            jax.ShapeDtypeStruct((1, node_count), f32),
        ),
        in_specs=[pl.BlockSpec(memory_space=pltpu.HBM)] * 7,
        out_specs=(vmem, vmem, vmem),
        scratch_shapes=[
            pltpu.SMEM(split_feature.shape, jnp.int32),
            pltpu.SMEM(split_bin.shape, jnp.int32),
            pltpu.VMEM(binned.shape, jnp.int32),
            pltpu.VMEM(gradients.shape, gradients.dtype),
            pltpu.VMEM(hessians.shape, hessians.dtype),
            pltpu.VMEM((1, rows_here), jnp.int32),
            pltpu.VMEM(elected.shape, jnp.int32),
            pltpu.VMEM((slots_here, rows_here), jnp.int32),
            pltpu.VMEM((1, rows_here), f32),
            pltpu.VMEM((n_rep - 1, 1, rows_here), f32),
            pltpu.VMEM((n_rows, 2, owned // pieces, LANES), jnp.int32),
            pltpu.VMEM((n_rows, 2, owned // pieces, LANES), jnp.int32),
            pltpu.VMEM((n_rows, owned, rows_here), jnp.int32),
            pltpu.VMEM((n_rows, owned, rows_here), jnp.int32),
            pltpu.VMEM((n_rep, n_rows, n_rep + 3, 1, rows_here // n_rep), f32),
            pltpu.VMEM((2, rows_here), f32),
            pltpu.VMEM((n_rows, 2 * node_count, rows_here), jnp.bfloat16),
            pltpu.VMEM((owned * BINS, rows_here), jnp.float8_e4m3fn),
            pltpu.VMEM((2 * node_count, owned * BINS), f32),
            pltpu.VMEM((1, node_count), f32),
            pltpu.VMEM((n_rows * n_rep - 1, 1, node_count), f32),
            dma((7,)),
        ]
        + [dma(())] * 2
        + [dma((1,))] * 4
        + [dma(())] * 2
        + [dma((parts + ends,)), dma(((n_rows - 2) * parts + ends,))]
        + [dma(())] * 2,
        compiler_params=pltpu.CompilerParams(collective_id=0, has_side_effects=True, vmem_limit_bytes=16 * 2**20),
    )(*(pltpu.with_memory_space_constraint(a, pltpu.HBM) for a in args))
    new_nodes, best, node_best = pl.pallas_call(
        hand_on,
        out_shape=tuple(jax.ShapeDtypeStruct(a.shape, a.dtype) for a in made),
        in_specs=[vmem] * 3,
        out_specs=(vmem,) * 3,
        compiler_params=pltpu.CompilerParams(vmem_limit_bytes=2**20),
    )(*made)
    return (
        new_nodes.reshape(rows_here),
        best.T.reshape(node_count, 1, owned),
        node_best.reshape(node_count),
    )


def solution(mesh):
    return jax.shard_map(
        functools.partial(body, mesh.shape["rows"], mesh.shape["rep"]),
        mesh=mesh,
        in_specs=(P("rows", "rep"), P("rows"), P("rows"), P("rows"), P(), P(), P(None, "rep")),
        out_specs=(P("rows"), P(None, "rep", "rows"), P()),
        check_vma=False,
    )
```

```python
import functools

import jax
import jax.numpy as jnp
from jax import lax
from jax.experimental import pallas as pl
from jax.experimental.pallas import tpu as pltpu
from jax.sharding import PartitionSpec as P

BINS = 128
LANES = 128
MESH = pl.DeviceIdType.MESH

l2_penalty = 1.0


def partner_of(n_rows, me, d):
    if n_rows & (n_rows - 1):
        return lax.rem(me + d, n_rows) if d else me
    other = me
    for bit in range(n_rows.bit_length()):
        if d >> bit & 1:
            other = other + (1 - 2 * lax.rem(me // 2**bit, 2)) * 2**bit
    return other


def parts_of(pieces, owned, rows_here):
    everything = slice(0, owned), slice(0, rows_here)
    if pieces == 1:
        return [everything], [[everything]]
    share = owned // pieces
    step = max(rows_here // 4, 2 * LANES)
    upper, lower = slice(0, share), slice(share, owned)
    usual = [(upper, slice(0, rows_here)), (lower, slice(LANES, rows_here))]
    last = [[(upper, slice(0, step)), (lower, slice(LANES, step))]]
    for begin in range(step, rows_here, step):
        last.append([(slice(0, owned), slice(begin, min(begin + step, rows_here)))])
    return usual, last


def kernel(
    n_rows, n_rep, pieces, issue, arrive,
    split_feature_in, split_bin_in, binned_in, gradients_in, hessians_in, parents_in, elected_in,
    new_nodes, best_out, node_best,
    split_feature, split_bin, binned, gradients, hessians, parents, elected, both_bins,
    side_snd, side_rcv, guess_snd, guess_rcv, bins_snd, bins_rcv, early, own_gh, weights, le, acc, top_snd, top_rcv,
    in_sems, side_ss, side_rs, early_ss, early_rs, fan_ss, fan_rs, guess_ss, guess_rs, bins_ss, bins_rs, top_ss, top_rs,
):
    rows_here, block_width = binned.shape
    node_count, slots_here = elected.shape
    parent_count = split_feature.shape[0]
    owned = slots_here // n_rows
    part_rows = rows_here // n_rep
    me = lax.axis_index("rows")
    rep = lax.axis_index("rep")
    slot_of = {d: s for s, d in enumerate(arrive, 1)}
    share = owned // pieces
    parts, steps = parts_of(pieces, owned, rows_here)
    ends = [part for step in steps for part in step]
    hedged = slice(owned - share, owned)
    groups = [(1, n_rows)]

    def at(d, e):
        return (partner_of(n_rows, me, d), lax.rem(rep + e, n_rep))

    def remote(src, dst, ss, rs, device):
        return pltpu.make_async_remote_copy(
            src_ref=src, dst_ref=dst, send_sem=ss, recv_sem=rs, device_id=device, device_id_type=MESH
        )

    def all_of(ref, ss, rs):
        return remote(ref, ref, ss, rs, at(1, 0))

    with jax.named_scope("load"):
        barrier = pltpu.get_barrier_semaphore()
        greeted = [(0, e) for e in range(1, n_rep)] + [(d, 0) for d in issue]
        for d, e in greeted:
            pl.semaphore_signal(barrier, inc=1, device_id=at(d, e), device_id_type=MESH)

        loads = []
        for i, (src, dst) in enumerate(
            (
                (split_feature_in, split_feature), (split_bin_in, split_bin), (parents_in, parents),
                (binned_in, binned),
                (gradients_in, gradients), (hessians_in, hessians), (elected_in, elected),
            )
        ):
            loads.append(pltpu.make_async_copy(src, dst, in_sems.at[i]))
            loads[-1].start()
        for load in loads[:3]:
            load.wait()

    with jax.named_scope("side"):
        parent_sub = lax.broadcasted_iota(jnp.int32, (parent_count, block_width), 0)
        column = lax.broadcasted_iota(jnp.int32, (parent_count, block_width), 1) + rep * block_width
        feature_of = jnp.zeros((parent_count, block_width), jnp.int32)
        parent_row = lax.broadcasted_iota(jnp.int32, (parent_count, rows_here), 0)
        bin_of = jnp.zeros((parent_count, rows_here), jnp.int32)
        owns = jnp.zeros((parent_count, rows_here), jnp.int32)
        low = rep * block_width
        for p in range(parent_count):
            feature = split_feature[p]
            owned_here = jnp.where((feature >= low) & (feature < low + block_width), 1, 0)
            feature_of = jnp.where(parent_sub == p, feature, feature_of)
            bin_of = jnp.where(parent_row == p, split_bin[p], bin_of)
            owns = jnp.where(parent_row == p, owned_here, owns)
        for load in loads[3:4]:
            load.wait()
        picks = jnp.where(feature_of == column, 1.0, 0.0).astype(jnp.bfloat16)
        values = lax.dot_general(
            picks,
            binned[...].astype(jnp.float32).astype(jnp.bfloat16),
            (((1,), (1,)), ((), ())),
            preferred_element_type=jnp.float32,
        )
        own_parents = parents[...]
        goes = (parent_row == own_parents) & (owns > 0) & (values > bin_of.astype(jnp.float32))
        side = jnp.sum(jnp.where(goes, 1.0, 0.0), axis=0, keepdims=True)
        side_snd[...] = side
        for load in loads[4:6]:
            load.wait()
        own_gh[0:1] = gradients[...].astype(jnp.float32).reshape(1, rows_here)
        own_gh[1:2] = hessians[...].astype(jnp.float32).reshape(1, rows_here)
        mine = pl.ds(pl.multiple_of(rep * part_rows, part_rows), part_rows)
        for f in range(n_rep):
            early[0, 0, f] = side[:, f * part_rows : (f + 1) * part_rows]
        early[0, 0, n_rep] = own_gh[0:1, mine]
        early[0, 0, n_rep + 1] = own_gh[1:2, mine]
        early[0, 0, n_rep + 2] = parents[:, mine].astype(jnp.float32)

    with jax.named_scope("barwait"):
        pl.semaphore_wait(barrier, len(greeted))
        for e in range(1, n_rep):
            remote(side_snd, side_rcv.at[e - 1], side_ss, side_rs, at(0, e)).start()
        for d in issue[::-1]:
            s = slot_of[d]
            g = [i for i, (low, high) in enumerate(groups) if low <= s < high][0]
            remote(early.at[0, 0], early.at[0, s], early_ss.at[g], early_rs.at[g], at(d, 0)).start()

    with jax.named_scope("gather"):
        loads[6].wait()
        elected_wide = elected[...].astype(jnp.float32).astype(jnp.bfloat16)

        def gather(begin, end):
            here = slice(begin, end)
            node_tile = lax.broadcasted_iota(jnp.int32, (node_count, end - begin), 0)
            above = 2 * own_parents[:, here]
            pieces_here = [
                binned[here, start * LANES : (start + 1) * LANES] for start in range(block_width // LANES)
            ]
            tables = [
                pieces_here[g] + (pieces_here[g + 1] * 256 if g + 1 < len(pieces_here) else 0)
                for g in range(0, len(pieces_here), 2)
            ]
            packed = None
            for child in range(2):
                child_hot = jnp.where(node_tile == above + child, 1.0, 0.0).astype(jnp.bfloat16)
                index = lax.dot_general(
                    child_hot, elected_wide, (((0,), (0,)), ((), ())), preferred_element_type=jnp.float32
                ).astype(jnp.int32)
                lane = index & (LANES - 1)
                part = lax.shift_right_logical(index, LANES.bit_length() - 1)
                chosen = None
                for g, table in enumerate(tables):
                    found = jnp.take_along_axis(table, lane, axis=1, mode="promise_in_bounds")
                    found = lax.shift_right_logical(found, (part & 1) * 8) & 255
                    chosen = found if chosen is None else jnp.where(part // 2 == g, found, chosen)
                packed = chosen if packed is None else packed + chosen * 256
            both_bins[:, here] = packed.T

        gather(0, LANES)
        if pieces > 1:
            for j in range(n_rows):
                two = both_bins[j * owned + owned - share : (j + 1) * owned, 0:LANES]
                guess_snd[j, 0] = two & 255
                guess_snd[j, 1] = lax.shift_right_logical(two, 8)
            for d in issue[::-1]:
                remote(
                    guess_snd.at[partner_of(n_rows, me, d)], guess_rcv.at[slot_of[d]], guess_ss, guess_rs, at(d, 0)
                ).start()
        gather(LANES, rows_here)

    with jax.named_scope("sidex"):
        sides = all_of(side_rcv, side_ss, side_rs)
        sides.wait_recv()
        for e in range(1, n_rep):
            side = side + side_rcv[e - 1]
        side = side.astype(jnp.int32)
        nodes = 2 * parents[...] + side
        new_nodes[...] = nodes

    with jax.named_scope("select"):
        shift = side * 8
        for j in range(n_rows):
            slots = slice(j * owned, (j + 1) * owned)
            bins_snd[j] = lax.shift_right_logical(both_bins[slots, :], jnp.broadcast_to(shift, (owned, rows_here))) & 255
        for d in issue:
            s = slot_of[d]
            for i, (slots, rows) in enumerate(ends if s == n_rows - 1 else parts):
                remote(
                    bins_snd.at[partner_of(n_rows, me, d), slots, rows], bins_rcv.at[s, slots, rows],
                    bins_ss.at[i + (len(parts) if s == n_rows - 1 else 0)], bins_rs.at[(s - 1) * len(parts) + i], at(d, 0),
                ).start()
        bins_rcv[0] = bins_snd[me]

    def early_of(g):
        return all_of(early.at[0, groups[g][0] : groups[g][1]], early_ss.at[g], early_rs.at[g])

    def fan_of(g):
        return all_of(early.at[1:n_rep, groups[g][0] : groups[g][1]], fan_ss.at[g], fan_rs.at[g])

    def fan(g):
        early_of(g).wait_recv()
        some = slice(*groups[g])
        for e in range(1, n_rep):
            remote(early.at[0, some], early.at[e, some], fan_ss.at[g], fan_rs.at[g], at(0, e)).start()

    with jax.named_scope("nodew"):
        fan(0)

    bin_sub = lax.broadcasted_iota(jnp.int32, (BINS, rows_here), 0).astype(jnp.float32).astype(jnp.bfloat16)
    node_sub = lax.broadcasted_iota(jnp.int32, (node_count, rows_here), 0)
    one = jnp.ones((), jnp.bfloat16)
    none = jnp.zeros((), jnp.bfloat16)
    acc[...] = jnp.zeros_like(acc)

    def weigh(node, grad, hess):
        there = node_sub == node
        return jnp.concatenate([jnp.where(there, grad, 0.0), jnp.where(there, hess, 0.0)], axis=0).astype(jnp.bfloat16)

    weights[0] = weigh(nodes, own_gh[0:1], own_gh[1:2])

    def arrived(s, i):
        slots, rows = parts[i]
        all_of(bins_rcv.at[s, slots, rows], bins_ss.at[i], bins_rs.at[(s - 1) * len(parts) + i]).wait_recv()

    def ended(i):
        slots, rows = ends[i]
        return all_of(
            bins_rcv.at[n_rows - 1, slots, rows], bins_ss.at[len(parts) + i], bins_rs.at[(n_rows - 2) * len(parts) + i]
        )

    def add(s, slots, rows):
        bins = bins_rcv[s, slots, rows].astype(jnp.float32).astype(jnp.bfloat16)
        cols = slice(slots.start * BINS, slots.stop * BINS)
        for k in range(slots.stop - slots.start):
            at_k = slice((slots.start + k) * BINS, (slots.start + k + 1) * BINS)
            le[at_k, rows] = jnp.where(bins[k : k + 1] <= bin_sub[:, rows], one, none).astype(le.dtype)
        acc[:, cols] += lax.dot_general(
            weights[s, :, rows], le[cols, rows], (((1,), (1,)), ((), ())), preferred_element_type=jnp.float32
        )

    guesses = all_of(guess_rcv.at[1:n_rows], guess_ss, guess_rs) if pieces > 1 else None

    def fill(g):
        fan_of(g).wait_recv()

        @pl.loop(*groups[g])
        def _(u):
            above, right, grad, hess = [], [], [], []
            for f in range(n_rep):
                e = lax.rem(rep + n_rep - f, n_rep)
                above.append(early[e, u, n_rep + 2])
                right.append(sum(early[c, u, f] for c in range(n_rep)))
                grad.append(early[e, u, n_rep])
                hess.append(early[e, u, n_rep + 1])
            above, right, grad, hess = (jnp.concatenate(x, axis=1) for x in (above, right, grad, hess))
            weights[u] = weigh((2.0 * above + right).astype(jnp.int32), grad, hess)
            if pieces > 1:
                bins_rcv[u, hedged, 0:LANES] = jnp.where(right[:, 0:LANES] > 0.5, guess_rcv[u, 1], guess_rcv[u, 0])

    everything = slice(0, rows_here)
    with jax.named_scope("own"):
        for piece in range(pieces):
            add(0, slice(piece * share, (piece + 1) * share), everything)
        for g in range(1, len(groups)):
            fan(g)
        if pieces > 1:
            guesses.wait_recv()
    with jax.named_scope("fill"):
        fill(0)

    with jax.named_scope("loop"):
        @pl.loop(1, n_rows - 1)
        def _(s):
            for piece in range(pieces):
                with jax.named_scope("w"):
                    arrived(s, piece)
                add(s, slice(piece * share, (piece + 1) * share), everything)

    i = 0
    for step in steps:
        with jax.named_scope("last"):
            with jax.named_scope("lw"):
                for _ in step:
                    ended(i).wait_recv()
                    i += 1
            add(n_rows - 1, slice(0, owned), slice(0 if step is steps[0] else step[0][1].start, step[0][1].stop))

    lane = lax.broadcasted_iota(jnp.int32, (node_count, LANES), 1)
    tops = jnp.full((node_count, LANES), -jnp.inf, jnp.float32)
    total_grad = total_hess = base = None
    for piece in range(pieces):
        with jax.named_scope("gain"):
            for k in range(share):
                cols = slice((piece * share + k) * BINS, (piece * share + k + 1) * BINS)
                left_grad = acc[0:node_count, cols]
                left_hess = acc[node_count : 2 * node_count, cols]
                if total_grad is None:
                    total_grad = jnp.broadcast_to(left_grad[:, BINS - 1 : BINS], left_grad.shape)
                    total_hess = jnp.broadcast_to(left_hess[:, BINS - 1 : BINS], left_hess.shape)
                    base = total_grad * total_grad / (total_hess + l2_penalty)
                right_grad = total_grad - left_grad
                gain = 0.5 * (
                    left_grad * left_grad / (left_hess + l2_penalty)
                    + right_grad * right_grad / (total_hess - left_hess + l2_penalty)
                    - base
                )
                top = jnp.max(jnp.where(lane < BINS - 1, gain, -jnp.inf), axis=1, keepdims=True)
                tops = jnp.where(lane == piece * share + k, top, tops)
    turned = tops.T
    best_out[...] = turned[0:owned]
    best = jnp.max(turned[0:owned], axis=0, keepdims=True)
    top_snd[...] = best

    with jax.named_scope("top"):
        others = [(d, e) for d in (*issue, 0) for e in range(n_rep) if d or e]
        for i, (d, e) in enumerate(others):
            remote(top_snd, top_rcv.at[i], top_ss, top_rs, at(d, e)).start()
        tops_all = all_of(top_rcv, top_ss, top_rs)
        tops_all.wait_recv()
        for i in range(len(others)):
            best = jnp.maximum(best, top_rcv[i])
        node_best[...] = best
        for sent in (sides, tops_all, *map(early_of, range(len(groups))), *map(fan_of, range(len(groups)))):
            sent.wait_send()
        if pieces > 1:
            guesses.wait_send()
        if n_rows > 2:
            for i, (slots, rows) in enumerate(parts):
                all_of(bins_rcv.at[1 : n_rows - 1, slots, rows], bins_ss.at[i], bins_rs.at[0]).wait_send()
        for i in range(len(ends)):
            ended(i).wait_send()


def hand_on(*refs):
    for src, dst in zip(refs[:3], refs[3:]):
        dst[...] = src[...]


def body(n_rows, n_rep, binned, gradients, hessians, parents, split_feature, split_bin, elected):
    rows_here, block_width = binned.shape
    node_count, slots_here = elected.shape
    owned = slots_here // n_rows
    pieces = 2 if owned % 16 == 0 and rows_here > 2 * LANES else 1
    parts, steps = parts_of(pieces, owned, rows_here)
    parts, ends = len(parts), sum(map(len, steps))
    f32 = jnp.float32
    vmem = pl.BlockSpec(memory_space=pltpu.VMEM)
    dma = pltpu.SemaphoreType.DMA
    order = tuple(range(1, n_rows))
    args = (split_feature, split_bin, binned, gradients, hessians, parents.reshape(1, rows_here), elected)
    made = pl.pallas_call(
        functools.partial(kernel, n_rows, n_rep, pieces, order, order),
        out_shape=(
            jax.ShapeDtypeStruct((1, rows_here), jnp.int32),
            jax.ShapeDtypeStruct((owned, node_count), f32),
            jax.ShapeDtypeStruct((1, node_count), f32),
        ),
        in_specs=[pl.BlockSpec(memory_space=pltpu.HBM)] * 7,
        out_specs=(vmem, vmem, vmem),
        scratch_shapes=[
            pltpu.SMEM(split_feature.shape, jnp.int32),
            pltpu.SMEM(split_bin.shape, jnp.int32),
            pltpu.VMEM(binned.shape, jnp.int32),
            pltpu.VMEM(gradients.shape, gradients.dtype),
            pltpu.VMEM(hessians.shape, hessians.dtype),
            pltpu.VMEM((1, rows_here), jnp.int32),
            pltpu.VMEM(elected.shape, jnp.int32),
            pltpu.VMEM((slots_here, rows_here), jnp.int32),
            pltpu.VMEM((1, rows_here), f32),
            pltpu.VMEM((n_rep - 1, 1, rows_here), f32),
            pltpu.VMEM((n_rows, 2, owned // pieces, LANES), jnp.int32),
            pltpu.VMEM((n_rows, 2, owned // pieces, LANES), jnp.int32),
            pltpu.VMEM((n_rows, owned, rows_here), jnp.int32),
            pltpu.VMEM((n_rows, owned, rows_here), jnp.int32),
            pltpu.VMEM((n_rep, n_rows, n_rep + 3, 1, rows_here // n_rep), f32),
            pltpu.VMEM((2, rows_here), f32),
            pltpu.VMEM((n_rows, 2 * node_count, rows_here), jnp.bfloat16),
            pltpu.VMEM((owned * BINS, rows_here), jnp.float8_e4m3fn),
            pltpu.VMEM((2 * node_count, owned * BINS), f32),
            pltpu.VMEM((1, node_count), f32),
            pltpu.VMEM((n_rows * n_rep - 1, 1, node_count), f32),
            dma((7,)),
        ]
        + [dma(())] * 2
        + [dma((1,))] * 4
        + [dma(())] * 2
        + [dma((parts + ends,)), dma(((n_rows - 2) * parts + ends,))]
        + [dma(())] * 2,
        compiler_params=pltpu.CompilerParams(collective_id=0, has_side_effects=True, vmem_limit_bytes=16 * 2**20),
    )(*(pltpu.with_memory_space_constraint(a, pltpu.HBM) for a in args))
    new_nodes, best, node_best = pl.pallas_call(
        hand_on,
        out_shape=tuple(jax.ShapeDtypeStruct(a.shape, a.dtype) for a in made),
        in_specs=[vmem] * 3,
        out_specs=(vmem,) * 3,
        compiler_params=pltpu.CompilerParams(vmem_limit_bytes=2**20),
    )(*made)
    return (
        new_nodes.reshape(rows_here),
        best.T.reshape(node_count, 1, owned),
        node_best.reshape(node_count),
    )


def solution(mesh):
    return jax.shard_map(
        functools.partial(body, mesh.shape["rows"], mesh.shape["rep"]),
        mesh=mesh,
        in_specs=(P("rows", "rep"), P("rows"), P("rows"), P("rows"), P(), P(), P(None, "rep")),
        out_specs=(P("rows"), P(None, "rep", "rows"), P()),
        check_vma=False,
    )
```
